1024 devices in a mesh: group: 2 (over core), dp: 32 (over z_lo, y), section: 4 (over x), tensor: 4 (over z_hi).
Axes of the slice: x: 4, y: 4, z: 32 (z_hi: 4, z_lo: 8; z = z_hi * 8 + z_lo), core: 2. Of those that a mesh axis runs over, the one named last changes fastest.
Arguments:
- merged: bfloat16 [6144, 5120], P('dp'), may hold values from -6 to 6
- counts: int32 [64], P('dp'), may hold values from 4 to 384
- owners: int32 [6144, 1], P('dp'), may hold values from 0 to 31; in each aligned block of 192 rows (0 to 191, 192 to 383, ...) at most 12 rows name the same one
- w_merge: bfloat16 [5120, 8192], P(None, ('group', 'section', 'tensor')), may hold values from -0.078125 to 0.078125
- norm_gain: float32 [8192], P(('group', 'section', 'tensor')), may hold values from 0.25 to 1.75
- cotangent: bfloat16 [32, 32, 12, 8192], P('dp', None, None, ('group', 'section', 'tensor')), may hold values from -6 to 6
Outputs:
- embedded: bfloat16 [32, 32, 12, 8192], P('dp', None, None, ('group', 'section', 'tensor'))
- grad_merged: float32 [6144, 5120], P('dp', ('group', 'section', 'tensor'))
- grad_weight: float32 [5120, 8192], P('dp', ('group', 'section', 'tensor'))
The draws below stay inside these ranges and needn't reach their ends.
Inputs may be any that keep to these rules, and one draw needn't show every extreme that they name: `owners`: in each replica's 192 rows no owner appears more than 12 times.
All inputs are finite; a program needn't handle non-finite values.
Results may differ from the reference program's by a relative error of at most 0.0049.
Values may be sent and summed in bfloat16 or wider, within the bound.
No kernel may reach another device: no remote copies, remote signals or barrier semaphores. Data moves between devices by JAX's collectives and lax.ppermute only.
A program may use at most 64 MiB of HBM per device.

```python
import math
import jax
import jax.numpy as jnp
import numpy as np
from jax import lax

D = 8192
DM = 5120
ROWS = 192
SAMP = 2
SLOT = 96
MOST = 12
N_DP = 32


def set_ends(values, key, smallest, top_value):
    place = [jax.random.randint(jax.random.fold_in(key, axis), (), 0, length) for axis, length in enumerate(values.shape)]
    widest = values.shape.index(max(values.shape))
    next_to = place[:widest] + [(place[widest] + 1) % values.shape[widest]] + place[widest + 1:]
    return values.at[tuple(place)].set(smallest).at[tuple(next_to)].set(top_value)


def block_scale(rng, dims, shards, least, largest):
    def one(dim, shards_of):
        steps = jax.random.uniform(jax.random.fold_in(jax.random.fold_in(rng, 6), dim), (shards_of,), jnp.float32, least / len(shards), largest / len(shards))
        return jnp.repeat(jnp.exp(steps), dims[dim] // shards_of).reshape((-1,) + (1,) * (len(dims) - dim - 1))

    gain = one(*shards[0])
    for cut in shards[1:]:
        gain = gain * one(*cut)
    return gain


def assign_block(stream_key, own, number, rows, count, top, most, lean):
    order = jax.random.permutation(stream_key, count)
    heavy_load, usual = shares(count, rows * top, most, lean, True), shares(count, rows * top, most, lean, False)
    places = jnp.arange(count)

    def named(tallies, offset_by):
        used = int((tallies > 0).sum())
        fixed = max(1, used // 4)
        passed = fixed + (places - fixed + offset_by * (used - fixed)) % max(1, count - fixed)
        return jnp.zeros((count,), jnp.int32).at[order[jnp.where(places < fixed, places, passed)]].set(jnp.asarray(tallies, jnp.int32))

    tallies = jnp.where(number % 4 == 0, named(heavy_load, number // 4), named(usual, number - number // 4 - 1))
    mixed = jax.random.permutation(jax.random.fold_in(own, 3), count)
    donor, sink = mixed[0:count // 2 * 2:2], mixed[1:count // 2 * 2:2]
    room = jnp.minimum(tallies[donor] - 1, most - tallies[sink]) // 2
    room = jnp.where((donor == order[0]) | (sink == order[0]) | (tallies[sink] == 0), 0, jnp.maximum(room, 0))
    passed = jax.random.randint(jax.random.fold_in(own, 4), (count // 2,), 0, 1 << 20) % (room + 1)
    tallies = tallies.at[donor].add(-passed).at[sink].add(passed)
    items = jnp.searchsorted(jnp.cumsum(tallies), jnp.arange(rows * top), side="right").astype(jnp.int32)
    table = items.reshape(top, rows).T
    table = table[jax.random.permutation(jax.random.fold_in(own, 1), rows)]
    offset_by = jax.random.randint(jax.random.fold_in(own, 2), (rows, 1), 0, top)
    return jnp.take_along_axis(table, (jnp.arange(top)[None, :] + offset_by) % top, axis=1)


def shares(amount, total, limit, slope, full):
    portions = [(1 << 20) // math.isqrt(rank ** slope) + 1 for rank in range(1, amount + 1)]
    largest = limit if full else min(limit, max(-(-total // amount), total * portions[0] // sum(portions)))
    least = 1 if total - largest >= amount - 1 else 0
    given, spare = [largest] + [least] * (amount - 1), total - largest - least * (amount - 1)
    while spare > 0:
        candidates = [i for i in range(1, amount) if given[i] < largest] or [i for i in range(1, amount) if given[i] < limit]
        pool, left = sum([portions[i] for i in candidates]), spare
        for i in candidates:
            extra = min(limit - given[i], max(1, left * portions[i] // pool), spare)
            given[i] = given[i] + extra
            spare = spare - extra
    return np.array(given)


def centred(key, dims, spread, most, split=(), kind=jnp.bfloat16):
    drawn = jax.random.normal(key, dims, jnp.float32) * spread
    if len(split) > 0:
        drawn = block_scale(key, dims, split, -0.22, 0.18) * drawn
    return jnp.clip(drawn, min=-most, max=most).astype(kind)


def setup_inputs(seed: int = 0) -> dict:
    key_list = jax.random.split(jax.random.key(seed), 7)
    merged = centred(key_list[0], (N_DP * ROWS, DM), 1.0, 6.0, ((0, 32),))
    counts = set_ends(jax.random.randint(key_list[1], (N_DP * SAMP,), 4, 4 * SLOT + 1), jax.random.fold_in(key_list[1], 1), 4, 4 * SLOT).astype(jnp.int32)
    owners_keys = jax.random.split(jax.random.fold_in(key_list[2], 1), (N_DP * ROWS) // ROWS)
    owners_turns = jax.random.permutation(jax.random.fold_in(key_list[2], 3), (N_DP * ROWS) // ROWS)
    owners = jax.vmap(lambda own, number: assign_block(jax.random.fold_in(key_list[2], 2), own, number, ROWS, N_DP, 1, MOST, 2))(owners_keys, owners_turns).reshape((N_DP * ROWS, 1))
    w_merge = centred(key_list[3], (DM, D), DM ** -0.5, 0.078125, ((1, 32),))
    norm_gain = jnp.clip(1.0 + 0.15 * jax.random.normal(key_list[4], (D,), jnp.float32), 0.25, 1.75)
    cotangent = centred(key_list[5], (N_DP, N_DP, MOST, D), 1.0, 6.0, ((0, 32), (3, 32)))
    return {"merged": merged, "counts": counts, "owners": owners, "w_merge": w_merge, "norm_gain": norm_gain, "cotangent": cotangent}


def reference(merged, counts, owners, w_merge, norm_gain, cotangent):
    total = merged.shape[0]
    projected = jnp.dot(merged, w_merge, preferred_element_type=jnp.float32).astype(jnp.bfloat16)
    row_index = jnp.arange(total, dtype=jnp.int32)
    within = row_index % ROWS
    image = row_index // ROWS * SAMP + within // SLOT
    valid = (4 * (within % SLOT) < counts[image]).astype(jnp.float32)
    masked = (projected.astype(jnp.float32) * valid[:, None]).astype(jnp.bfloat16)
    owner = owners[:, 0].astype(jnp.int32)
    hits = (owner[:, None] == jnp.arange(N_DP, dtype=jnp.int32)[None, :]).astype(jnp.int32)
    blocked = hits.reshape(N_DP, ROWS, N_DP)
    before = jnp.cumsum(blocked, axis=1) - blocked
    slot_index = lax.optimization_barrier(jnp.sum(before * blocked, axis=2)).reshape(total).astype(jnp.int32)
    block = (row_index // ROWS).astype(jnp.int32)
    values = masked.astype(jnp.float32)
    scale = jax.lax.rsqrt(lax.optimization_barrier(jnp.mean(values * values, axis=1)) + 1e-05)
    normed = (values * scale[:, None] * norm_gain[None, :]).astype(jnp.bfloat16)
    embedded = jnp.zeros((N_DP, N_DP, MOST, D), jnp.bfloat16).at[owner, block, slot_index].set(normed)
    grad_in = cotangent[owner, block, slot_index].astype(jnp.float32) * norm_gain[None, :]
    inner = lax.optimization_barrier(jnp.mean(grad_in * values, axis=1))
    back = (scale[:, None] * grad_in - values * (scale ** 3 * inner)[:, None]).astype(jnp.bfloat16)
    back = (back.astype(jnp.float32) * valid[:, None]).astype(jnp.bfloat16)
    grad_merged = jnp.dot(back, w_merge.T, preferred_element_type=jnp.float32)
    grad_weight = jnp.dot(merged.T, back, preferred_element_type=jnp.float32)
    return (embedded, grad_merged, grad_weight)
```

```python
import jax
import jax.numpy as jnp
from jax import lax
from jax.sharding import Mesh, PartitionSpec as P

D = 8192
BF16 = jnp.bfloat16
F32 = jnp.float32
FEATURES = ("group", "section", "tensor")
REPLICAS = ("near", "y")
Y_CHIPS = 4


def routing(owners, replicas, slots):
    rows = owners.shape[0]
    owner = owners[:, 0]
    index = jnp.arange(rows, dtype=jnp.int32)
    earlier = (owner[:, None] == owner[None, :]) & (index[:, None] < index[None, :])
    slot_index = jnp.sum(earlier.astype(jnp.int32), axis=0)
    target = owner * slots + slot_index
    every = jnp.arange(replicas * slots, dtype=jnp.int32)
    return (every[:, None] == target[None, :]).astype(BF16)


def valid_rows(counts, rows):
    images = counts.shape[0]
    per_image = rows // images
    row_index = jnp.arange(rows, dtype=jnp.int32)
    picked = (row_index // per_image)[:, None] == jnp.arange(images, dtype=jnp.int32)[None, :]
    count_of = jnp.sum(jnp.where(picked, counts[None, :], 0), axis=1)
    return (4 * (row_index % per_image) < count_of).astype(F32)[:, None]


def dot(a, b, contract):
    return lax.dot_general(a, b, (contract, ((), ())), preferred_element_type=F32)


def added(pieces):
    total = pieces[0].astype(F32)
    for piece in pieces[1:]:
        total = total + piece.astype(F32)
    return total


def on_device(merged, counts, owners, w_merge, norm_gain, cotangent):
    rows, hidden = merged.shape
    columns = w_merge.shape[1]
    slots = cotangent.shape[2]
    near = lax.axis_size("near")
    far = lax.axis_size("y")
    replicas = near * far
    groups = lax.axis_size("group")
    gain = norm_gain[None, :]

    arrived = lax.all_to_all(cotangent[0], REPLICAS, split_axis=0, concat_axis=0, tiled=True)

    valid = valid_rows(counts, rows)
    placer = routing(owners, replicas, slots)
    projected = dot(merged, w_merge, ((1,), (0,))).astype(BF16)
    masked = (projected.astype(F32) * valid).astype(BF16)
    arrived, masked = lax.optimization_barrier((arrived, masked))
    values = masked.astype(F32)

    taken = dot(placer, arrived.reshape(replicas * slots, columns), ((0,), (0,)))
    grad_in = taken * gain
    sums = jnp.stack([jnp.sum(values * values, axis=1), jnp.sum(grad_in * values, axis=1)])
    for axis in FEATURES:
        sums = lax.psum(sums, axis)
    scale = lax.rsqrt(sums[0] / D + 1e-05)[:, None]
    inner = (sums[1] / D)[:, None]
    back = (scale * grad_in - values * (scale**3 * inner)).astype(BF16)
    back = (back.astype(F32) * valid).astype(BF16)

    half = hidden // groups
    mine = lax.axis_index("group")
    other_w = lax.dynamic_slice_in_dim(w_merge, (1 - mine) * half, half, 0)
    own_w = lax.dynamic_slice_in_dim(w_merge, mine * half, half, 0)
    away = dot(back, other_w, ((1,), (1,))).astype(BF16)
    partner = lax.ppermute(away, "group", [(0, 1), (1, 0)])
    terms = dot(back, own_w, ((1,), (1,))) + partner.astype(F32)
    terms, back = lax.optimization_barrier((terms, back))
    terms = lax.psum_scatter(terms, "section", scatter_dimension=1, tiled=True)
    grad_merged = lax.psum_scatter(terms, "tensor", scatter_dimension=1, tiled=True)

    weight_terms = dot(merged, back, ((0,), (0,))).astype(BF16)
    share = hidden // replicas
    weight_terms = weight_terms.reshape(near, far, share, columns).swapaxes(0, 1)
    weight_terms = lax.all_to_all(weight_terms, "y", 0, 0, tiled=True)
    weight_terms = added(weight_terms).astype(BF16)
    weight_terms = lax.all_to_all(weight_terms, "near", 0, 0, tiled=True)
    weight_terms, scale = lax.optimization_barrier((weight_terms, scale))
    grad_weight = added(weight_terms)

    normed = (values * scale * gain).astype(BF16)
    outgoing = dot(placer, normed, ((1,), (0,))).astype(BF16)
    outgoing = outgoing.reshape(replicas, slots, columns)
    embedded = lax.all_to_all(outgoing, REPLICAS, split_axis=0, concat_axis=0, tiled=True)
    return (embedded[None], grad_merged, grad_weight)


def solution(mesh):
    shape = mesh.devices.shape
    devices = mesh.devices.reshape(shape[0], shape[1] // Y_CHIPS, Y_CHIPS, shape[2], shape[3])
    inner = Mesh(devices, ("group", "near", "y", "section", "tensor"))
    return jax.shard_map(
        on_device,
        mesh=inner,
        in_specs=(
            P(REPLICAS, None),
            P(REPLICAS),
            P(REPLICAS, None),
            P(None, FEATURES),
            P(FEATURES),
            P(REPLICAS, None, None, FEATURES),
        ),
        out_specs=(
            P(REPLICAS, None, None, FEATURES),
            P(REPLICAS, FEATURES),
            P(REPLICAS, FEATURES),
        ),
        check_vma=False,
    )
```

```python
import jax
import jax.numpy as jnp
from jax import lax
from jax.sharding import Mesh, PartitionSpec as P

D = 8192
BF16 = jnp.bfloat16
F32 = jnp.float32
FEATURES = ("group", "section", "tensor")
REPLICAS = ("near", "y")
Y_CHIPS = 4


def routing(owners, replicas, slots):
    rows = owners.shape[0]
    owner = owners[:, 0]
    index = jnp.arange(rows, dtype=jnp.int32)
    earlier = (owner[:, None] == owner[None, :]) & (index[:, None] < index[None, :])
    slot_index = jnp.sum(earlier.astype(jnp.int32), axis=0)
    target = owner * slots + slot_index
    every = jnp.arange(replicas * slots, dtype=jnp.int32)
    return (every[:, None] == target[None, :]).astype(BF16)


def valid_rows(counts, rows):
    images = counts.shape[0]
    per_image = rows // images
    row_index = jnp.arange(rows, dtype=jnp.int32)
    picked = (row_index // per_image)[:, None] == jnp.arange(images, dtype=jnp.int32)[None, :]
    count_of = jnp.sum(jnp.where(picked, counts[None, :], 0), axis=1)
    return (4 * (row_index % per_image) < count_of).astype(F32)[:, None]


def dot(a, b, contract):
    return lax.dot_general(a, b, (contract, ((), ())), preferred_element_type=F32)


def added(pieces):
    total = pieces[0].astype(F32)
    for piece in pieces[1:]:
        total = total + piece.astype(F32)
    return total


LANES = 128


def folded(w, shares):
    wide = w.shape[0] // shares
    return w.reshape(shares, 2, wide // 2, -1).swapaxes(1, 2).reshape(shares * wide // 2, -1)


def dense_terms(which, half, back, w, w_folded, shares):
    wide = 2 * half // shares
    top, rest = back[:LANES], back[LANES:]
    empty = jnp.zeros_like(rest)
    both = jnp.concatenate(
        [jnp.concatenate([rest, empty], axis=1), jnp.concatenate([empty, rest], axis=1)], axis=0
    )
    plain = dot(lax.dynamic_slice_in_dim(w, which * half, half, 0), top, ((1,), (1,)))
    fold = dot(lax.dynamic_slice_in_dim(w_folded, which * (half // 2), half // 2, 0), both, ((1,), (1,)))
    return jnp.concatenate(
        [plain.reshape(-1, wide, LANES), fold.reshape(-1, wide // 2, LANES)], axis=1
    )


def unfolded(dense):
    wide = 2 * dense.shape[0] // 3
    fold = dense[wide:]
    rest = jnp.concatenate([fold[:, : LANES // 2], fold[:, LANES // 2 :]], axis=0)
    return jnp.concatenate([dense[:wide], rest], axis=1).T


def on_device(merged, counts, owners, w_merge, norm_gain, cotangent):
    rows, hidden = merged.shape
    columns = w_merge.shape[1]
    slots = cotangent.shape[2]
    near = lax.axis_size("near")
    far = lax.axis_size("y")
    replicas = near * far
    groups = lax.axis_size("group")
    gain = norm_gain[None, :]

    arrived = lax.all_to_all(cotangent[0], REPLICAS, split_axis=0, concat_axis=0, tiled=True)

    sections = lax.axis_size("section")
    pieces = groups * sections
    part = rows // pieces
    mine = lax.axis_index("group")
    piece = lax.dynamic_slice_in_dim(merged, (mine * sections + lax.axis_index("section")) * part, part, 0)
    piece = piece.reshape(part, near, hidden // near).swapaxes(0, 1)

    valid = valid_rows(counts, rows)
    placer = routing(owners, replicas, slots)
    projected = dot(merged, w_merge, ((1,), (0,))).astype(BF16)
    masked = (projected.astype(F32) * valid).astype(BF16)
    shares = groups * sections * lax.axis_size("tensor")
    w_folded = folded(w_merge, shares)
    arrived, masked, piece, w_folded = lax.optimization_barrier((arrived, masked, piece, w_folded))
    block = lax.all_to_all(piece, "near", 0, 0, tiled=True)
    values = masked.astype(F32)

    taken = dot(placer, arrived.reshape(replicas * slots, columns), ((0,), (0,)))
    grad_in = taken * gain
    sums = jnp.stack([jnp.sum(values * values, axis=1), jnp.sum(grad_in * values, axis=1)])
    for axis in FEATURES:
        sums = lax.psum(sums, axis)
    sums, block = lax.optimization_barrier((sums, block))
    scale = lax.rsqrt(sums[0] / D + 1e-05)[:, None]
    inner = (sums[1] / D)[:, None]
    back = (scale * grad_in - values * (scale**3 * inner)).astype(BF16)
    back = (back.astype(F32) * valid).astype(BF16)

    half = hidden // groups
    away = dense_terms(1 - mine, half, back, w_merge, w_folded, shares).astype(BF16)
    partner = lax.ppermute(away, "group", [(0, 1), (1, 0)])
    terms = dense_terms(mine, half, back, w_merge, w_folded, shares) + partner.astype(F32)
    terms, back = lax.optimization_barrier((terms, back))
    terms = lax.psum_scatter(terms, "section", scatter_dimension=0, tiled=True)

    copies = jnp.broadcast_to(back[None], (near, *back.shape))
    near_back = lax.all_to_all(copies, "near", 0, 0, tiled=True)
    block, near_back = lax.optimization_barrier((block, near_back))
    block = lax.all_gather(block, "section", axis=0)
    block, terms = lax.optimization_barrier((block, terms))
    grad_merged = unfolded(lax.psum_scatter(terms, "tensor", scatter_dimension=0, tiled=True)[0])
    others = lax.ppermute(block, "group", [(0, 1), (1, 0)])
    near_back = near_back.reshape(near, groups, pieces // groups, part, columns)
    near_back = near_back.transpose(1, 2, 0, 3, 4).reshape(groups, -1, columns)
    width = hidden // near
    first = lax.dynamic_index_in_dim(near_back, mine, 0, keepdims=False)
    second = lax.dynamic_index_in_dim(near_back, 1 - mine, 0, keepdims=False)
    weight_terms = dot(block.reshape(-1, width), first, ((0,), (0,)))
    weight_terms = weight_terms + dot(others.reshape(-1, width), second, ((0,), (0,)))
    weight_terms = weight_terms.astype(BF16).reshape(far, width // far, columns)
    weight_terms = lax.all_to_all(weight_terms, "y", 0, 0, tiled=True)
    weight_terms, scale = lax.optimization_barrier((weight_terms, scale))
    grad_weight = added(weight_terms)

    normed = (values * scale * gain).astype(BF16)
    outgoing = dot(placer, normed, ((1,), (0,))).astype(BF16)
    outgoing = outgoing.reshape(replicas, slots, columns)
    embedded = lax.all_to_all(outgoing, REPLICAS, split_axis=0, concat_axis=0, tiled=True)
    return (embedded[None], grad_merged, grad_weight)


def solution(mesh):
    shape = mesh.devices.shape
    devices = mesh.devices.reshape(shape[0], shape[1] // Y_CHIPS, Y_CHIPS, shape[2], shape[3])
    inner = Mesh(devices, ("group", "near", "y", "section", "tensor"))
    return jax.shard_map(
        on_device,
        mesh=inner,
        in_specs=(
            P(REPLICAS, None),
            P(REPLICAS),
            P(REPLICAS, None),
            P(None, FEATURES),
            P(FEATURES),
            P(REPLICAS, None, None, FEATURES),
        ),
        out_specs=(
            P(REPLICAS, None, None, FEATURES),
            P(REPLICAS, FEATURES),
            P(REPLICAS, FEATURES),
        ),
        check_vma=False,
    )
```

```python
import jax
import jax.numpy as jnp
from jax import lax
from jax.sharding import Mesh, PartitionSpec as P

D = 8192
BF16 = jnp.bfloat16
F32 = jnp.float32
FEATURES = ("group", "section", "tensor")
REPLICAS = ("half", "quad", "y")
QUAD = 4
Y_CHIPS = 4


def routing(owners, replicas, slots):
    rows = owners.shape[0]
    owner = owners[:, 0]
    index = jnp.arange(rows, dtype=jnp.int32)
    earlier = (owner[:, None] == owner[None, :]) & (index[:, None] < index[None, :])
    slot_index = jnp.sum(earlier.astype(jnp.int32), axis=0)
    target = owner * slots + slot_index
    every = jnp.arange(replicas * slots, dtype=jnp.int32)
    return (every[:, None] == target[None, :]).astype(BF16)


def valid_rows(counts, rows):
    images = counts.shape[0]
    per_image = rows // images
    row_index = jnp.arange(rows, dtype=jnp.int32)
    picked = (row_index // per_image)[:, None] == jnp.arange(images, dtype=jnp.int32)[None, :]
    count_of = jnp.sum(jnp.where(picked, counts[None, :], 0), axis=1)
    return (4 * (row_index % per_image) < count_of).astype(F32)[:, None]


def dot(a, b, contract):
    return lax.dot_general(a, b, (contract, ((), ())), preferred_element_type=F32)


def added(pieces):
    total = pieces[0].astype(F32)
    for piece in pieces[1:]:
        total = total + piece.astype(F32)
    return total


LANES = 128


def folded(w, shares):
    wide = w.shape[0] // shares
    return w.reshape(shares, 2, wide // 2, -1).swapaxes(1, 2).reshape(shares * wide // 2, -1)


def dense_terms(which, half, back, w, w_folded, shares):
    wide = 2 * half // shares
    top, rest = back[:LANES], back[LANES:]
    empty = jnp.zeros_like(rest)
    both = jnp.concatenate(
        [jnp.concatenate([rest, empty], axis=1), jnp.concatenate([empty, rest], axis=1)], axis=0
    )
    plain = dot(lax.dynamic_slice_in_dim(w, which * half, half, 0), top, ((1,), (1,)))
    fold = dot(lax.dynamic_slice_in_dim(w_folded, which * (half // 2), half // 2, 0), both, ((1,), (1,)))
    return jnp.concatenate(
        [plain.reshape(-1, wide, LANES), fold.reshape(-1, wide // 2, LANES)], axis=1
    )


def unfolded(dense):
    wide = 2 * dense.shape[0] // 3
    fold = dense[wide:]
    rest = jnp.concatenate([fold[:, : LANES // 2], fold[:, LANES // 2 :]], axis=0)
    return jnp.concatenate([dense[:wide], rest], axis=1).T


def on_device(merged, counts, owners, w_merge, norm_gain, cotangent):
    rows, hidden = merged.shape
    columns = w_merge.shape[1]
    slots = cotangent.shape[2]
    halves = lax.axis_size("half")
    quad = lax.axis_size("quad")
    far = lax.axis_size("y")
    replicas = halves * quad * far
    groups = lax.axis_size("group")
    gain = norm_gain[None, :]

    arrived = lax.all_to_all(cotangent[0], REPLICAS, split_axis=0, concat_axis=0, tiled=True)

    sections = lax.axis_size("section")
    pieces = groups * sections
    part = rows // pieces
    mine = lax.axis_index("group")
    piece = lax.dynamic_slice_in_dim(merged, (mine * sections + lax.axis_index("section")) * part, part, 0)
    piece = piece.reshape(part, halves, quad, -1).transpose(2, 0, 1, 3)
    piece = piece.reshape(quad, part, -1)

    valid = valid_rows(counts, rows)
    placer = routing(owners, replicas, slots)
    projected = dot(merged, w_merge, ((1,), (0,))).astype(BF16)
    masked = (projected.astype(F32) * valid).astype(BF16)
    shares = groups * sections * lax.axis_size("tensor")
    w_folded = folded(w_merge, shares)
    arrived, masked, piece, w_folded = lax.optimization_barrier((arrived, masked, piece, w_folded))
    block = lax.all_to_all(piece, "quad", 0, 0, tiled=True)
    values = masked.astype(F32)

    taken = dot(placer, arrived.reshape(replicas * slots, columns), ((0,), (0,)))
    grad_in = taken * gain
    sums = jnp.stack([jnp.sum(values * values, axis=1), jnp.sum(grad_in * values, axis=1)])
    for axis in FEATURES:
        sums = lax.psum(sums, axis)
    sums, block = lax.optimization_barrier((sums, block))
    scale = lax.rsqrt(sums[0] / D + 1e-05)[:, None]
    inner = (sums[1] / D)[:, None]
    back = (scale * grad_in - values * (scale**3 * inner)).astype(BF16)
    back = (back.astype(F32) * valid).astype(BF16)

    half = hidden // groups
    away = dense_terms(1 - mine, half, back, w_merge, w_folded, shares).astype(BF16)
    partner = lax.ppermute(away, "group", [(0, 1), (1, 0)])
    terms = dense_terms(mine, half, back, w_merge, w_folded, shares) + partner.astype(F32)
    terms, back = lax.optimization_barrier((terms, back))
    terms = lax.psum_scatter(terms, "section", scatter_dimension=0, tiled=True)

    copies = jnp.broadcast_to(back[None], (quad, *back.shape))
    quad_back = lax.all_to_all(copies, "quad", 0, 0, tiled=True)
    quad_back, scale = lax.optimization_barrier((quad_back, scale))

    normed = (values * scale * gain).astype(BF16)
    outgoing = dot(placer, normed, ((1,), (0,))).astype(BF16)
    outgoing = outgoing.reshape(replicas, slots, columns)
    outgoing, block = lax.optimization_barrier((outgoing, block))
    embedded = lax.all_to_all(outgoing, REPLICAS, split_axis=0, concat_axis=0, tiled=True)

    block = lax.all_gather(block, "section", axis=0)
    terms = terms.astype(BF16)
    block, terms, embedded = lax.optimization_barrier((block, terms, embedded))
    terms = lax.psum_scatter(terms, "tensor", scatter_dimension=0, tiled=True)
    grad_merged = unfolded(terms[0].astype(F32))
    others = lax.ppermute(block, "group", [(0, 1), (1, 0)])
    quad_back = quad_back.reshape(quad, groups, sections, part, columns)
    quad_back = quad_back.transpose(1, 2, 0, 3, 4).reshape(groups, -1, columns)
    first = lax.dynamic_index_in_dim(quad_back, mine, 0, keepdims=False)
    second = lax.dynamic_index_in_dim(quad_back, 1 - mine, 0, keepdims=False)
    weight_terms = dot(block.reshape(-1, block.shape[-1]), first, ((0,), (0,)))
    weight_terms = weight_terms + dot(others.reshape(-1, block.shape[-1]), second, ((0,), (0,)))
    weight_terms = weight_terms.astype(BF16).reshape(halves, far, -1, columns).swapaxes(0, 1)
    weight_terms = lax.all_to_all(weight_terms, "y", 0, 0, tiled=True)
    weight_terms = added(weight_terms)
    here = lax.axis_index("half")
    away = lax.dynamic_index_in_dim(weight_terms, 1 - here, 0, keepdims=False).astype(BF16)
    kept = lax.dynamic_index_in_dim(weight_terms, here, 0, keepdims=False)
    across = lax.ppermute(away, "half", [(0, 1), (1, 0)])
    grad_weight = kept + across.astype(F32)
    return (embedded[None], grad_merged, grad_weight)


def solution(mesh):
    shape = mesh.devices.shape
    devices = mesh.devices.reshape(shape[0], -1, QUAD, Y_CHIPS, shape[2], shape[3])
    inner = Mesh(devices, ("group", *REPLICAS, "section", "tensor"))
    return jax.shard_map(
        on_device,
        mesh=inner,
        in_specs=(
            P(REPLICAS, None),
            P(REPLICAS),
            P(REPLICAS, None),
            P(None, FEATURES),
            P(FEATURES),
            P(REPLICAS, None, None, FEATURES),
        ),
        out_specs=(
            P(REPLICAS, None, None, FEATURES),
            P(REPLICAS, FEATURES),
            P(REPLICAS, FEATURES),
        ),
        check_vma=False,
    )
```

```python
import jax
import jax.numpy as jnp
from jax import lax
from jax.sharding import Mesh, PartitionSpec as P

D = 8192
BF16 = jnp.bfloat16
F32 = jnp.float32
FEATURES = ("group", "section", "tensor")
REPLICAS = ("half", "quad", "y")
QUAD = 4
Y_CHIPS = 4


def routing(owners, replicas, slots):
    rows = owners.shape[0]
    owner = owners[:, 0]
    index = jnp.arange(rows, dtype=jnp.int32)
    earlier = (owner[:, None] == owner[None, :]) & (index[:, None] < index[None, :])
    slot_index = jnp.sum(earlier.astype(jnp.int32), axis=0)
    target = owner * slots + slot_index
    every = jnp.arange(replicas * slots, dtype=jnp.int32)
    return (every[:, None] == target[None, :]).astype(BF16)


def valid_rows(counts, rows):
    images = counts.shape[0]
    per_image = rows // images
    row_index = jnp.arange(rows, dtype=jnp.int32)
    picked = (row_index // per_image)[:, None] == jnp.arange(images, dtype=jnp.int32)[None, :]
    count_of = jnp.sum(jnp.where(picked, counts[None, :], 0), axis=1)
    return (4 * (row_index % per_image) < count_of).astype(F32)[:, None]


def dot(a, b, contract):
    return lax.dot_general(a, b, (contract, ((), ())), preferred_element_type=F32)


def added(pieces):
    total = pieces[0].astype(F32)
    for piece in pieces[1:]:
        total = total + piece.astype(F32)
    return total


def reduced(pieces, axis, dim):
    size = lax.axis_size(axis)
    here = lax.axis_index(axis)
    received = [lax.dynamic_index_in_dim(pieces, here, dim, keepdims=False)]
    for step in range(1, size):
        piece = lax.dynamic_index_in_dim(pieces, (here + step) % size, dim, keepdims=False)
        received.append(lax.ppermute(piece, axis, [(i, (i + step) % size) for i in range(size)]))
    return added(received)


LANES = 128


def folded(w, shares):
    wide = w.shape[0] // shares
    return w.reshape(shares, 2, wide // 2, -1).swapaxes(1, 2).reshape(shares * wide // 2, -1)


def dense_terms(which, half, back, w, w_folded, shares):
    wide = 2 * half // shares
    top, rest = back[:LANES], back[LANES:]
    empty = jnp.zeros_like(rest)
    both = jnp.concatenate(
        [jnp.concatenate([rest, empty], axis=1), jnp.concatenate([empty, rest], axis=1)], axis=0
    )
    plain = dot(lax.dynamic_slice_in_dim(w, which * half, half, 0), top, ((1,), (1,)))
    fold = dot(lax.dynamic_slice_in_dim(w_folded, which * (half // 2), half // 2, 0), both, ((1,), (1,)))
    return jnp.concatenate(
        [plain.reshape(-1, wide, LANES), fold.reshape(-1, wide // 2, LANES)], axis=1
    )


def unfolded(dense):
    wide = 2 * dense.shape[0] // 3
    fold = dense[wide:]
    rest = jnp.concatenate([fold[:, : LANES // 2], fold[:, LANES // 2 :]], axis=0)
    return jnp.concatenate([dense[:wide], rest], axis=1).T


def on_device(merged, counts, owners, w_merge, norm_gain, cotangent):
    rows, hidden = merged.shape
    columns = w_merge.shape[1]
    slots = cotangent.shape[2]
    halves = lax.axis_size("half")
    quad = lax.axis_size("quad")
    far = lax.axis_size("y")
    replicas = halves * quad * far
    groups = lax.axis_size("group")
    gain = norm_gain[None, :]

    arrived = lax.all_to_all(cotangent[0], REPLICAS, split_axis=0, concat_axis=0, tiled=True)

    sections = lax.axis_size("section")
    pieces = groups * sections
    part = rows // pieces
    mine = lax.axis_index("group")
    piece = lax.dynamic_slice_in_dim(merged, (mine * sections + lax.axis_index("section")) * part, part, 0)
    piece = piece.reshape(part, halves, quad, -1).transpose(2, 0, 1, 3)
    piece = piece.reshape(quad, part, -1)

    valid = valid_rows(counts, rows)
    placer = routing(owners, replicas, slots)
    projected = dot(merged, w_merge, ((1,), (0,))).astype(BF16)
    masked = (projected.astype(F32) * valid).astype(BF16)
    shares = groups * sections * lax.axis_size("tensor")
    w_folded = folded(w_merge, shares)
    arrived, masked, piece, w_folded = lax.optimization_barrier((arrived, masked, piece, w_folded))
    block = lax.all_to_all(piece, "quad", 0, 0, tiled=True)
    values = masked.astype(F32)

    taken = dot(placer, arrived.reshape(replicas * slots, columns), ((0,), (0,)))
    grad_in = taken * gain
    sums = jnp.stack([jnp.sum(values * values, axis=1), jnp.sum(grad_in * values, axis=1)])
    for axis in FEATURES:
        sums = lax.psum(sums, axis)
    sums, block = lax.optimization_barrier((sums, block))
    scale = lax.rsqrt(sums[0] / D + 1e-05)[:, None]
    inner = (sums[1] / D)[:, None]
    back = (scale * grad_in - values * (scale**3 * inner)).astype(BF16)
    back = (back.astype(F32) * valid).astype(BF16)

    copies = jnp.broadcast_to(back[None], (quad, *back.shape))
    quad_back = lax.all_to_all(copies, "quad", 0, 0, tiled=True)

    half = hidden // groups
    away = dense_terms(1 - mine, half, back, w_merge, w_folded, shares).astype(BF16)
    partner = lax.ppermute(away, "group", [(0, 1), (1, 0)])
    terms = dense_terms(mine, half, back, w_merge, w_folded, shares) + partner.astype(F32)
    terms = terms.astype(BF16)
    terms, quad_back, block = lax.optimization_barrier((terms, quad_back, block))
    terms = lax.all_to_all(terms.reshape(sections, -1, LANES), "section", 0, 0, tiled=True)
    block = lax.all_gather(block, "section", axis=0)
    terms = added(terms).astype(BF16)
    terms, block = lax.optimization_barrier((terms, block))
    terms = lax.all_to_all(terms.reshape(lax.axis_size("tensor"), -1, LANES), "tensor", 0, 0, tiled=True)
    terms, scale = lax.optimization_barrier((terms, scale))
    grad_merged = unfolded(added(terms))

    normed = (values * scale * gain).astype(BF16)
    outgoing = dot(placer, normed, ((1,), (0,))).astype(BF16)
    outgoing = outgoing.reshape(replicas, slots, columns)
    embedded = lax.all_to_all(outgoing, REPLICAS, split_axis=0, concat_axis=0, tiled=True)

    others = lax.ppermute(block, "group", [(0, 1), (1, 0)])
    quad_back = quad_back.reshape(quad, groups, sections, part, columns)
    quad_back = quad_back.transpose(1, 2, 0, 3, 4).reshape(groups, -1, columns)
    first = lax.dynamic_index_in_dim(quad_back, mine, 0, keepdims=False)
    second = lax.dynamic_index_in_dim(quad_back, 1 - mine, 0, keepdims=False)
    weight_terms = dot(block.reshape(-1, block.shape[-1]), first, ((0,), (0,)))
    weight_terms = weight_terms + dot(others.reshape(-1, block.shape[-1]), second, ((0,), (0,)))
    weight_terms = weight_terms.astype(BF16).reshape(halves, far, -1, columns)
    weight_terms = reduced(weight_terms, "y", 1)
    grad_weight = reduced(weight_terms.astype(BF16), "half", 0)
    return (embedded[None], grad_merged, grad_weight)


def solution(mesh):
    shape = mesh.devices.shape
    devices = mesh.devices.reshape(shape[0], -1, QUAD, Y_CHIPS, shape[2], shape[3])
    inner = Mesh(devices, ("group", *REPLICAS, "section", "tensor"))
    return jax.shard_map(
        on_device,
        mesh=inner,
        in_specs=(
            P(REPLICAS, None),
            P(REPLICAS),
            P(REPLICAS, None),
            P(None, FEATURES),
            P(FEATURES),
            P(REPLICAS, None, None, FEATURES),
        ),
        out_specs=(
            P(REPLICAS, None, None, FEATURES),
            P(REPLICAS, FEATURES),
            P(REPLICAS, FEATURES),
        ),
        check_vma=False,
    )
```

```python
import jax
import jax.numpy as jnp
from jax import lax
from jax.experimental import pallas as pl
from jax.experimental.pallas import tpu as pltpu
from jax.sharding import Mesh, PartitionSpec as P

D = 8192
BF16 = jnp.bfloat16
F32 = jnp.float32
FEATURES = ("group", "section", "tensor")
REPLICAS = ("half", "quad", "y")
QUAD = 4
Y_CHIPS = 4


def routing(owners, replicas, slots):
    rows = owners.shape[0]
    owner = owners[:, 0]
    index = jnp.arange(rows, dtype=jnp.int32)
    earlier = (owner[:, None] == owner[None, :]) & (index[:, None] < index[None, :])
    slot_index = jnp.sum(earlier.astype(jnp.int32), axis=0)
    target = owner * slots + slot_index
    every = jnp.arange(replicas * slots, dtype=jnp.int32)
    return (every[:, None] == target[None, :]).astype(BF16)


def valid_rows(counts, rows):
    images = counts.shape[0]
    per_image = rows // images
    row_index = jnp.arange(rows, dtype=jnp.int32)
    picked = (row_index // per_image)[:, None] == jnp.arange(images, dtype=jnp.int32)[None, :]
    count_of = jnp.sum(jnp.where(picked, counts[None, :], 0), axis=1)
    return (4 * (row_index % per_image) < count_of).astype(F32)[:, None]


def dot(a, b, contract):
    return lax.dot_general(a, b, (contract, ((), ())), preferred_element_type=F32)


def added(pieces):
    total = pieces[0].astype(F32)
    for piece in pieces[1:]:
        total = total + piece.astype(F32)
    return total


def exchanged(pieces, axis, dim):
    size = lax.axis_size(axis)
    here = lax.axis_index(axis)
    received = [lax.dynamic_index_in_dim(pieces, here, dim, keepdims=False)]
    for step in range(1, size):
        piece = lax.dynamic_index_in_dim(pieces, (here + step) % size, dim, keepdims=False)
        received.append(lax.ppermute(piece, axis, [(i, (i + step) % size) for i in range(size)]))
    return received


def gathered(piece, axis):
    size = lax.axis_size(axis)
    received = [piece]
    for step in range(1, size):
        received.append(lax.ppermute(piece, axis, [(i, (i + step) % size) for i in range(size)]))
    return jnp.stack(received)


LANES = 128


def dense_body(which, w, back, *refs):
    out = refs[-1]
    wide = 2 * out.shape[1] // 3
    top, rest = back[:LANES], back[LANES:]
    empty = jnp.zeros_like(rest)
    plain = dot(w[...], top, ((1,), (1,)))
    left = dot(w[...], jnp.concatenate([rest, empty], axis=0), ((1,), (1,)))
    right = dot(w[...], jnp.concatenate([empty, rest], axis=0), ((1,), (1,)))
    for share in range(out.shape[0]):
        start = share * wide
        fold = left[start : start + wide // 2] + right[start + wide // 2 : start + wide]
        plain_share = plain[start : start + wide]
        if len(refs) == 2:
            plain_share = plain_share + refs[0][share, :wide].astype(F32)
            fold = fold + refs[0][share, wide:].astype(F32)
        out[share, :wide] = plain_share.astype(BF16)
        out[share, wide:] = fold.astype(BF16)


def dense_terms(which, back, w, shares, groups, steps, *partner):
    hidden, columns = w.shape
    wide = hidden // shares
    here = shares // groups
    block = (here // steps, 3 * wide // 2, LANES)
    tile = pl.BlockSpec(block, lambda i, which: (i, 0, 0))
    return pl.pallas_call(
        dense_body,
        out_shape=jax.ShapeDtypeStruct((here, *block[1:]), BF16),
        grid_spec=pltpu.PrefetchScalarGridSpec(
            num_scalar_prefetch=1,
            grid=(steps,),
            in_specs=[
                pl.BlockSpec((hidden // groups // steps, columns), lambda i, which: (which[0] * steps + i, 0)),
                pl.BlockSpec(back.shape, lambda i, which: (0, 0)),
                *(tile for _ in partner),
            ],
            out_specs=tile,
        ),
        name="dense_terms",
    )(which[None], w, back, *partner)


def unfolded(dense):
    wide = 2 * dense.shape[0] // 3
    fold = dense[wide:]
    rest = jnp.concatenate([fold[:, : LANES // 2], fold[:, LANES // 2 :]], axis=0)
    return jnp.concatenate([dense[:wide], rest], axis=1).T


def on_device(merged, counts, owners, w_merge, norm_gain, cotangent):
    rows, _ = merged.shape
    columns = w_merge.shape[1]
    slots = cotangent.shape[2]
    halves = lax.axis_size("half")
    quad = lax.axis_size("quad")
    far = lax.axis_size("y")
    replicas = halves * quad * far
    groups = lax.axis_size("group")
    gain = norm_gain[None, :]

    arrived = lax.all_to_all(cotangent[0], REPLICAS, split_axis=0, concat_axis=0, tiled=True)

    sections = lax.axis_size("section")
    pieces = groups * sections
    part = rows // pieces
    mine = lax.axis_index("group")
    piece = lax.dynamic_slice_in_dim(merged, (mine * sections + lax.axis_index("section")) * part, part, 0)
    piece = piece.reshape(part, halves, quad, -1).transpose(2, 0, 1, 3)
    piece = piece.reshape(quad, part, -1)

    valid = valid_rows(counts, rows)
    placer = routing(owners, replicas, slots)
    projected = dot(merged, w_merge, ((1,), (0,))).astype(BF16)
    masked = (projected.astype(F32) * valid).astype(BF16)
    shares = groups * sections * lax.axis_size("tensor")
    block = jnp.stack(exchanged(piece, "quad", 0))
    arrived, masked, _ = lax.optimization_barrier((arrived, masked, block))
    block = gathered(block, "section")
    values = masked.astype(F32)

    taken = dot(placer, arrived.reshape(replicas * slots, columns), ((0,), (0,)))
    grad_in = taken * gain
    sums = jnp.stack([jnp.sum(values * values, axis=1), jnp.sum(grad_in * values, axis=1)])
    for axis in FEATURES:
        sums = lax.psum(sums, axis)
    sums, block = lax.optimization_barrier((sums, block))
    scale = lax.rsqrt(sums[0] / D + 1e-05)[:, None]
    inner = (sums[1] / D)[:, None]
    back = (scale * grad_in - values * (scale**3 * inner)).astype(BF16)
    back = (back.astype(F32) * valid).astype(BF16)

    tensors = lax.axis_size("tensor")
    away = dense_terms(1 - mine, back, w_merge, shares, groups, sections)
    partner = lax.ppermute(away, "group", [(0, 1), (1, 0)])
    terms = dense_terms(mine, back, w_merge, shares, groups, sections, partner)
    terms, back, scale = lax.optimization_barrier((terms, back, scale))
    terms = lax.all_to_all(terms.reshape(sections, -1, LANES), "section", 0, 0, tiled=True)

    quad_back = gathered(back, "quad")
    normed = (values * scale * gain).astype(BF16)
    outgoing = dot(placer, normed, ((1,), (0,))).astype(BF16)
    outgoing = outgoing.reshape(replicas, slots, columns)

    terms = added(terms).astype(BF16)
    terms, block, quad_back, outgoing = lax.optimization_barrier((terms, block, quad_back, outgoing))
    terms = lax.all_to_all(terms.reshape(tensors, -1, LANES), "tensor", 0, 0, tiled=True)

    others = lax.ppermute(block, "group", [(0, 1), (1, 0)])
    quad_back = quad_back.reshape(quad, groups, sections, part, columns)
    beside = lax.axis_index("section")
    quad_back = [
        lax.dynamic_index_in_dim(quad_back, (beside - step) % sections, 2, keepdims=False)
        for step in range(sections)
    ]
    quad_back = jnp.stack(quad_back).transpose(2, 0, 1, 3, 4).reshape(groups, -1, columns)
    first = lax.dynamic_index_in_dim(quad_back, mine, 0, keepdims=False)
    second = lax.dynamic_index_in_dim(quad_back, 1 - mine, 0, keepdims=False)
    weight_terms = dot(block.reshape(-1, block.shape[-1]), first, ((0,), (0,)))
    weight_terms = weight_terms + dot(others.reshape(-1, block.shape[-1]), second, ((0,), (0,)))
    weight_terms = weight_terms.astype(BF16).reshape(halves, far, -1, columns)
    weight_terms = added(exchanged(weight_terms, "y", 1)).astype(BF16)
    terms, outgoing = lax.optimization_barrier((terms, outgoing))
    grad_weight = added(exchanged(weight_terms, "half", 0))
    embedded = lax.all_to_all(outgoing, REPLICAS, split_axis=0, concat_axis=0, tiled=True)
    grad_merged = unfolded(added(terms))
    return (embedded[None], grad_merged, grad_weight)


def solution(mesh):
    shape = mesh.devices.shape
    devices = mesh.devices.reshape(shape[0], -1, QUAD, Y_CHIPS, shape[2], shape[3])
    inner = Mesh(devices, ("group", *REPLICAS, "section", "tensor"))
    return jax.shard_map(
        on_device,
        mesh=inner,
        in_specs=(
            P(REPLICAS, None),
            P(REPLICAS),
            P(REPLICAS, None),
            P(None, FEATURES),
            P(FEATURES),
            P(REPLICAS, None, None, FEATURES),
        ),
        out_specs=(
            P(REPLICAS, None, None, FEATURES),
            P(REPLICAS, FEATURES),
            P(REPLICAS, FEATURES),
        ),
        check_vma=False,
    )
```

```python
import jax
import jax.numpy as jnp
from jax import lax
from jax.experimental import pallas as pl
from jax.experimental.pallas import tpu as pltpu
from jax.sharding import Mesh, PartitionSpec as P

D = 8192
BF16 = jnp.bfloat16
F32 = jnp.float32
FEATURES = ("group", "section", "tensor")
REPLICAS = ("half", "quad", "y")
QUAD = 4
Y_CHIPS = 4


def routing(owners, replicas, slots):
    rows = owners.shape[0]
    owner = owners[:, 0]
    index = jnp.arange(rows, dtype=jnp.int32)
    earlier = (owner[:, None] == owner[None, :]) & (index[:, None] < index[None, :])
    slot_index = jnp.sum(earlier.astype(jnp.int32), axis=0)
    target = owner * slots + slot_index
    every = jnp.arange(replicas * slots, dtype=jnp.int32)
    return (every[:, None] == target[None, :]).astype(BF16)


def valid_rows(counts, rows):
    images = counts.shape[0]
    per_image = rows // images
    row_index = jnp.arange(rows, dtype=jnp.int32)
    picked = (row_index // per_image)[:, None] == jnp.arange(images, dtype=jnp.int32)[None, :]
    count_of = jnp.sum(jnp.where(picked, counts[None, :], 0), axis=1)
    return (4 * (row_index % per_image) < count_of).astype(F32)[:, None]


def dot(a, b, contract):
    return lax.dot_general(a, b, (contract, ((), ())), preferred_element_type=F32)


def added(pieces):
    total = pieces[0].astype(F32)
    for piece in pieces[1:]:
        total = total + piece.astype(F32)
    return total


def reduced(pieces, axis, dim):
    size = lax.axis_size(axis)
    here = lax.axis_index(axis)
    received = [lax.dynamic_index_in_dim(pieces, here, dim, keepdims=False)]
    for step in range(1, size):
        piece = lax.dynamic_index_in_dim(pieces, (here + step) % size, dim, keepdims=False)
        received.append(lax.ppermute(piece, axis, [(i, (i + step) % size) for i in range(size)]))
    return added(received)


def gathered(piece, axis):
    size = lax.axis_size(axis)
    here = lax.axis_index(axis)
    received = [piece]
    for step in range(1, size):
        received.append(lax.ppermute(piece, axis, [(i, (i + step) % size) for i in range(size)]))
    received = jnp.stack(received)
    return jnp.stack(
        [lax.dynamic_index_in_dim(received, (here - i) % size, 0, keepdims=False) for i in range(size)]
    )


LANES = 128


def dense_body(which, w, back, *refs):
    out = refs[-1]
    wide = 2 * out.shape[1] // 3
    top, rest = back[:LANES], back[LANES:]
    empty = jnp.zeros_like(rest)
    plain = dot(w[...], top, ((1,), (1,)))
    left = dot(w[...], jnp.concatenate([rest, empty], axis=0), ((1,), (1,)))
    right = dot(w[...], jnp.concatenate([empty, rest], axis=0), ((1,), (1,)))
    for share in range(out.shape[0]):
        start = share * wide
        fold = left[start : start + wide // 2] + right[start + wide // 2 : start + wide]
        plain_share = plain[start : start + wide]
        if len(refs) == 2:
            plain_share = plain_share + refs[0][share, :wide].astype(F32)
            fold = fold + refs[0][share, wide:].astype(F32)
        out[share, :wide] = plain_share.astype(BF16)
        out[share, wide:] = fold.astype(BF16)


def dense_terms(which, back, w, shares, groups, steps, *partner):
    hidden, columns = w.shape
    wide = hidden // shares
    here = shares // groups
    block = (here // steps, 3 * wide // 2, LANES)
    tile = pl.BlockSpec(block, lambda i, which: (i, 0, 0))
    return pl.pallas_call(
        dense_body,
        out_shape=jax.ShapeDtypeStruct((here, *block[1:]), BF16),
        grid_spec=pltpu.PrefetchScalarGridSpec(
            num_scalar_prefetch=1,
            grid=(steps,),
            in_specs=[
                pl.BlockSpec((hidden // groups // steps, columns), lambda i, which: (which[0] * steps + i, 0)),
                pl.BlockSpec(back.shape, lambda i, which: (0, 0)),
                *(tile for _ in partner),
            ],
            out_specs=tile,
        ),
        name="dense_terms",
    )(which[None], w, back, *partner)


def unfolded(dense):
    wide = 2 * dense.shape[0] // 3
    fold = dense[wide:]
    rest = jnp.concatenate([fold[:, : LANES // 2], fold[:, LANES // 2 :]], axis=0)
    return jnp.concatenate([dense[:wide], rest], axis=1).T


def on_device(merged, counts, owners, w_merge, norm_gain, cotangent):
    rows, _ = merged.shape
    columns = w_merge.shape[1]
    slots = cotangent.shape[2]
    halves = lax.axis_size("half")
    quad = lax.axis_size("quad")
    far = lax.axis_size("y")
    replicas = halves * quad * far
    groups = lax.axis_size("group")
    gain = norm_gain[None, :]

    arrived = lax.all_to_all(cotangent[0], REPLICAS, split_axis=0, concat_axis=0, tiled=True)

    sections = lax.axis_size("section")
    pieces = groups * sections
    part = rows // pieces
    mine = lax.axis_index("group")
    piece = lax.dynamic_slice_in_dim(merged, (mine * sections + lax.axis_index("section")) * part, part, 0)
    piece = piece.reshape(part, halves, quad, -1).transpose(2, 0, 1, 3)
    piece = piece.reshape(quad, part, -1)

    valid = valid_rows(counts, rows)
    placer = routing(owners, replicas, slots)
    projected = dot(merged, w_merge, ((1,), (0,))).astype(BF16)
    masked = (projected.astype(F32) * valid).astype(BF16)
    shares = groups * sections * lax.axis_size("tensor")
    arrived, masked, piece = lax.optimization_barrier((arrived, masked, piece))
    block = lax.all_to_all(piece, "quad", 0, 0, tiled=True)
    values = masked.astype(F32)

    taken = dot(placer, arrived.reshape(replicas * slots, columns), ((0,), (0,)))
    grad_in = taken * gain
    sums = jnp.stack([jnp.sum(values * values, axis=1), jnp.sum(grad_in * values, axis=1)])
    for axis in FEATURES:
        sums = lax.psum(sums, axis)
    sums, block = lax.optimization_barrier((sums, block))
    scale = lax.rsqrt(sums[0] / D + 1e-05)[:, None]
    inner = (sums[1] / D)[:, None]
    back = (scale * grad_in - values * (scale**3 * inner)).astype(BF16)
    back = (back.astype(F32) * valid).astype(BF16)

    tensors = lax.axis_size("tensor")
    away = dense_terms(1 - mine, back, w_merge, shares, groups, sections)
    partner = lax.ppermute(away, "group", [(0, 1), (1, 0)])
    terms = dense_terms(mine, back, w_merge, shares, groups, sections, partner)
    terms, back, scale = lax.optimization_barrier((terms, back, scale))
    terms = lax.all_to_all(terms.reshape(sections, -1, LANES), "section", 0, 0, tiled=True)

    quad_back = gathered(back, "quad")
    normed = (values * scale * gain).astype(BF16)
    outgoing = dot(placer, normed, ((1,), (0,))).astype(BF16)
    outgoing = outgoing.reshape(replicas, slots, columns)

    terms = added(terms).astype(BF16)
    terms, block, quad_back, outgoing = lax.optimization_barrier((terms, block, quad_back, outgoing))
    terms = lax.all_to_all(terms.reshape(tensors, -1, LANES), "tensor", 0, 0, tiled=True)
    block = lax.all_gather(block, "section", axis=0)
    others = lax.ppermute(block, "group", [(0, 1), (1, 0)])
    quad_back = quad_back.reshape(quad, groups, sections, part, columns)
    quad_back = quad_back.transpose(1, 2, 0, 3, 4).reshape(groups, -1, columns)
    first = lax.dynamic_index_in_dim(quad_back, mine, 0, keepdims=False)
    second = lax.dynamic_index_in_dim(quad_back, 1 - mine, 0, keepdims=False)
    weight_terms = dot(block.reshape(-1, block.shape[-1]), first, ((0,), (0,)))
    weight_terms = weight_terms + dot(others.reshape(-1, block.shape[-1]), second, ((0,), (0,)))
    weight_terms = weight_terms.astype(BF16).reshape(halves, far, -1, columns)
    weight_terms = reduced(weight_terms, "y", 1).astype(BF16)
    terms, outgoing = lax.optimization_barrier((terms, outgoing))
    grad_weight = reduced(weight_terms, "half", 0)
    embedded = lax.all_to_all(outgoing, REPLICAS, split_axis=0, concat_axis=0, tiled=True)
    grad_merged = unfolded(added(terms))
    return (embedded[None], grad_merged, grad_weight)


def solution(mesh):
    shape = mesh.devices.shape
    devices = mesh.devices.reshape(shape[0], -1, QUAD, Y_CHIPS, shape[2], shape[3])
    inner = Mesh(devices, ("group", *REPLICAS, "section", "tensor"))
    return jax.shard_map(
        on_device,
        mesh=inner,
        in_specs=(
            P(REPLICAS, None),
            P(REPLICAS),
            P(REPLICAS, None),
            P(None, FEATURES),
            P(FEATURES),
            P(REPLICAS, None, None, FEATURES),
        ),
        out_specs=(
            P(REPLICAS, None, None, FEATURES),
            P(REPLICAS, FEATURES),
            P(REPLICAS, FEATURES),
        ),
        check_vma=False,
    )
```
